32 devices in a mesh: gx: 4 (over x, core), gy: 8 (over z, y).
Axes of the slice: x: 2, y: 2, z: 4, core: 2. Of those that a mesh axis runs over, the one named last changes fastest.
Arguments:
- base: int32 [2, 3, 65536], P(None, None, ('gx', 'gy')), may hold values from -2 to 125, as said below
- offset: float32 [2, 3, 65536], P(None, None, ('gx', 'gy')), may hold values from 0.5 to 1.5
- velocity: float32 [3, 65536], P(None, ('gx', 'gy')), may hold values from -4 to 4
- affine: float32 [9, 65536], P(None, ('gx', 'gy')), may hold values from -3 to 3
- volume: float32 [65536], P(('gx', 'gy')), may hold values from 0.8 to 1.25
- node_mask: int32 [128, 128, 128], P('gx', 'gy'), may hold values 0 or 1
- direction: int32 [65536], P(('gx', 'gy')), may hold values from 0 to 8, as said below
Outputs:
- migrated: float32 [16, 98304], P(None, ('gx', 'gy'))
The draws below stay inside these ranges and needn't reach their ends.
Inputs may be any that keep to these rules, and one draw needn't show every extreme that they name: base[s, 0] lies in -2 to 31, base[s, 1] in -2 to 15, base[s, 2] in 0 to 125. Of one block column's rows, at most 128 carry any one direction other than 4; in every draw some block column has exactly 128 rows in some direction.
All inputs are finite; a program needn't handle non-finite values. No bound on the sum of `node_mask` on one device may be relied on, other than what follows from the above.
Results may differ from the reference program's by a relative error of at most 0.0003.
Values may be sent and summed in bfloat16 or wider, within the bound.
A program may use at most 64 MiB of HBM per device.

```python
import jax
import jax.numpy as jnp

CX = 32
CY = 16
NZ = 128
PART_DEV = 2048
CAP = 128
NX = 128
NY = 128
NPART = 65536
N_GX = 4
N_GY = 8


def draw_base(key, part):
    key_x, key_y, key_z = jax.random.split(key, 3)
    first = jax.random.randint(key_x, (2, 1, NPART), -2, CX)
    second = jax.random.randint(key_y, (2, 1, NPART), -2, CY)
    third = jax.random.randint(key_z, (2, 1, NPART), 0, NZ - 2)
    return jnp.concatenate([first, second, third], 1).astype(jnp.int32)


def draw_direction(key, part):
    groups = NPART // PART_DEV
    keys = jax.random.split(jax.random.fold_in(key, 17), 4)
    level = jax.random.randint(keys[0], (groups, 1), 1, 4)
    raw = jnp.minimum(jax.random.randint(keys[1], (groups, 8), 0, CAP // 3 + 1) * level, CAP)
    chosen = jax.random.randint(keys[2], (groups, 1), 0, 8)
    counts = jnp.where(jnp.arange(8)[None, :] == chosen, CAP, raw)
    bounds = jnp.cumsum(counts, 1)
    order = jax.vmap(lambda subkey: jax.random.permutation(subkey, PART_DEV))(jax.random.split(keys[3], groups))
    lane = jnp.sum((order[:, :, None] >= bounds[:, None, :]).astype(jnp.int32), 2)
    code = jnp.where(lane < 4, lane, jnp.where(lane < 8, lane + 1, 4))
    return code.reshape(NPART).astype(jnp.int32)


def set_ends(drawn, own_key, least, largest):
    shape = drawn.shape
    spot = [jax.random.randint(jax.random.fold_in(own_key, axis), (), 0, shape[axis]) for axis in range(len(shape))]
    drawn = drawn.at[tuple(spot)].set(least)
    longest = shape.index(max(shape))
    spot[longest] = (spot[longest] + 1) % shape[longest]
    return drawn.at[tuple(spot)].set(largest)


def block_levels(own_key, shape, cuts, smallest, high):
    def one(dim, shards_of):
        steps = jax.random.uniform(jax.random.fold_in(jax.random.fold_in(own_key, 6), dim), (shards_of,), jnp.float32, smallest / len(cuts), high / len(cuts))
        return jnp.repeat(jnp.exp(steps), shape[dim] // shards_of).reshape((-1,) + (1,) * (len(shape) - dim - 1))

    loudness = one(*cuts[0])
    for cut in cuts[1:]:
        loudness = loudness * one(*cut)
    return loudness


def scatter_about(rng, shape, scale, limit, shards=(), held_as=jnp.bfloat16):
    entries = jax.random.normal(rng, shape, jnp.float32) * scale
    if len(shards) > 0:
        entries = block_levels(rng, shape, shards, -0.22, 0.18) * entries
    return jnp.clip(entries, min=-limit, max=limit).astype(held_as)


def setup_inputs(seed: int = 0) -> dict:
    streams_of = jax.random.split(jax.random.key(seed), 8)
    base = draw_base(jax.random.fold_in(streams_of[7], 71), 0)
    offset = jnp.clip(0.5 + 1.0 * jax.random.uniform(streams_of[1], (2, 3, NPART), jnp.float32) ** block_levels(streams_of[1], (2, 3, NPART), ((2, 32),), -0.2, 0.2), 0.5, 1.5)
    velocity = scatter_about(streams_of[2], (3, NPART), 1.0, 4.0, ((1, 32),), jnp.float32)
    affine = scatter_about(streams_of[3], (9, NPART), 0.5, 3.0, ((1, 32),), jnp.float32)
    volume = jnp.clip(0.8 + 0.45 * jax.random.uniform(streams_of[4], (NPART,), jnp.float32) ** block_levels(streams_of[4], (NPART,), ((0, 32),), -0.2, 0.2), 0.8, 1.25)
    node_mask = set_ends((jax.random.randint(streams_of[5], (NX, NY, NZ), 0, 6) < 1).astype(jnp.int32), jax.random.fold_in(streams_of[5], 1), 0, 1)
    direction = draw_direction(jax.random.fold_in(streams_of[7], 71), 0)
    return {"base": base, "offset": offset, "velocity": velocity, "affine": affine, "volume": volume, "node_mask": node_mask, "direction": direction}


PARTICLE_MASS = 1.0
STIFFNESS = 4.0
TIME_STEP = 0.1
GRAVITY = 3.0
MASS_FLOOR = 0.5


def rounded(value):
    return value.astype(jnp.bfloat16).astype(jnp.float32)


def spline(frac):
    return [0.5 * (1.5 - frac) ** 2, 0.75 - (frac - 1.0) ** 2, 0.5 * (frac - 0.5) ** 2]


def substep(bases, offsets, velocity, affine, volume, keep, block_x, block_y):
    count = velocity.shape[1]
    start_x = (bases[0] + block_x * CX + 2).astype(jnp.int32)
    start_y = (bases[1] + block_y * CY + 2).astype(jnp.int32)
    start_z = bases[2].astype(jnp.int32)
    weights = [spline(offsets[axis]) for axis in range(3)]
    slopes = [[weights[axis][node] * (node - offsets[axis]) for node in range(3)] for axis in range(3)]
    stress = -STIFFNESS * (volume - 1.0)
    matrix = PARTICLE_MASS * affine.reshape(3, 3, count) + stress[None, None] * jnp.eye(3, dtype=jnp.float32)[:, :, None]
    zero_row = jnp.zeros((1, count), jnp.float32)
    moment = jnp.concatenate([PARTICLE_MASS * jnp.ones((1, count), jnp.float32), PARTICLE_MASS * velocity], 0)
    along = [jnp.concatenate([zero_row, matrix[:, axis]], 0) for axis in range(3)]
    grid = jnp.zeros((4, NX + 4, NY + 4, NZ), jnp.float32)
    for node_x in range(3):
        for node_y in range(3):
            plain = rounded(weights[0][node_x] * weights[1][node_y])
            slope_x = rounded(slopes[0][node_x] * weights[1][node_y])
            slope_y = rounded(weights[0][node_x] * slopes[1][node_y])
            for node_z in range(3):
                first = rounded(weights[2][node_z] * moment + slopes[2][node_z] * along[2])
                second = rounded(weights[2][node_z] * along[0])
                third = rounded(weights[2][node_z] * along[1])
                values = plain * first + slope_x * second + slope_y * third
                grid = grid.at[:, start_x + node_x, start_y + node_y, start_z + node_z].add(values)
    inner = grid[:, 2:NX + 2, 2:NY + 2]
    speed = inner[1:4] / jnp.maximum(inner[0], MASS_FLOOR)[None]
    speed = speed.at[2].add(-TIME_STEP * GRAVITY)
    speed = (speed * keep[None]).astype(jnp.bfloat16)
    padded = jnp.pad(speed, ((0, 0), (2, 2), (2, 2), (0, 0))).astype(jnp.float32)
    new_velocity = jnp.zeros((3, count), jnp.float32)
    part_x = jnp.zeros((3, count), jnp.float32)
    part_y = jnp.zeros((3, count), jnp.float32)
    part_z = jnp.zeros((3, count), jnp.float32)
    for node_x in range(3):
        for node_y in range(3):
            plain = rounded(weights[0][node_x] * weights[1][node_y])
            slope_x = rounded(slopes[0][node_x] * weights[1][node_y])
            slope_y = rounded(weights[0][node_x] * slopes[1][node_y])
            for node_z in range(3):
                nodal = padded[:, start_x + node_x, start_y + node_y, start_z + node_z]
                new_velocity = new_velocity + plain * nodal * weights[2][node_z]
                part_x = part_x + slope_x * nodal * weights[2][node_z]
                part_y = part_y + slope_y * nodal * weights[2][node_z]
                part_z = part_z + plain * nodal * slopes[2][node_z]
    new_affine = 4.0 * jnp.stack([part_x, part_y, part_z], 1).reshape(9, count)
    new_volume = volume * (1.0 + TIME_STEP * (new_affine[0] + new_affine[4] + new_affine[8]))
    return new_velocity, new_affine, new_volume


def reference(base, offset, velocity, affine, volume, node_mask, direction):
    devices = N_GX * N_GY
    count = velocity.shape[1]
    owner = (jnp.arange(count) // PART_DEV).astype(jnp.int32)
    block_x = owner // N_GY
    block_y = owner % N_GY
    keep = (1 - node_mask).astype(jnp.float32)
    state_v, state_c, state_j = velocity, affine, volume
    for sub in range(2):
        state_v, state_c, state_j = substep(base[sub], offset[sub], state_v, state_c, state_j, keep, block_x, block_y)
    position = base[1].astype(jnp.float32) + offset[1] + TIME_STEP * state_v
    step_x = direction // 3 - 1
    step_y = direction % 3 - 1
    inside = (block_x + step_x >= 0) & (block_x + step_x < N_GX) & (block_y + step_y >= 0) & (block_y + step_y < N_GY)
    moving = jnp.where(inside, direction, 4).astype(jnp.int32)
    step_x = jnp.where(inside, step_x, 0)
    step_y = jnp.where(inside, step_y, 0)
    shift_rows = jnp.stack([step_x * CX, step_y * CY, jnp.zeros_like(step_x)]).astype(jnp.float32)
    state = jnp.concatenate([position - shift_rows, state_v, state_c, state_j[None]], 0)
    lane = jnp.where(moving < 4, moving, moving - 1)
    hits = (jnp.arange(8, dtype=jnp.int32)[:, None] == lane[None]) & (moving != 4)[None]
    running = jnp.cumsum(hits.astype(jnp.int32).reshape(8, devices, PART_DEV), 2).reshape(8, count) - 1
    rank = jnp.sum(jnp.where(hits, running, 0), 0).astype(jnp.int32)
    width = PART_DEV + 8 * CAP
    target = (block_x + step_x) * N_GY + (block_y + step_y)
    local_row = (jnp.arange(count) % PART_DEV).astype(jnp.int32)
    slot = jnp.where(moving == 4, owner * width + local_row, target * width + PART_DEV + lane * CAP + rank).astype(jnp.int32)
    migrated = jnp.zeros((16, devices * width), jnp.float32).at[:, slot].set(state)
    return migrated
```

```python
import functools

import jax
import jax.numpy as jnp
import numpy as np
from jax import lax
from jax.experimental import pallas as pl
from jax.experimental.pallas import tpu as pltpu
from jax.sharding import PartitionSpec as P

PARTICLE_MASS = 1.0
STIFFNESS = 4.0
TIME_STEP = 0.1
GRAVITY = 3.0
MASS_FLOOR = 0.5
LANES = 128
OUTSIDE = -100

F32 = jnp.float32
BF16 = jnp.bfloat16
NT = (((1,), (1,)), ((), ()))

BLOCKS = ((0, -1), (0, 1), (-1, 0), (1, 0), (-1, -1), (-1, 1), (1, -1), (1, 1))
CORNER_ROWS = 16


def block_rows(size_x, size_y):
    counts = [2 * size_x] * 2 + [2 * size_y] * 2 + [CORNER_ROWS] * 4
    starts = [sum(counts[:place]) for place in range(8)]
    return (list(zip(starts, counts)), sum(counts))


def owner_rows(size_x, size_y):
    places, total = block_rows(size_x, size_y)
    rows = np.full(total, -1, np.int64)
    for (dx, dy), (start, _) in zip(BLOCKS, places):
        span_x = range(2) if dx else range(size_x)
        span_y = range(2) if dy else range(size_y)
        low_x = size_x - 2 if dx < 0 else 0
        low_y = size_y - 2 if dy < 0 else 0
        for x in span_x:
            for y in span_y:
                if dx and dy:
                    spot = 2 * x + y
                elif dx:
                    spot = x * size_y + y
                else:
                    spot = y * size_x + x
                rows[start + spot] = (low_x + x) * size_y + low_y + y
    return rows


def spline(frac):
    return [0.5 * (1.5 - frac) ** 2, 0.75 - (frac - 1.0) ** 2, 0.5 * (frac - 0.5) ** 2]


def pick(place, values):
    return jnp.where(
        place == 0,
        values[0],
        jnp.where(place == 1, values[1], jnp.where(place == 2, values[2], 0.0)),
    )


def weights_of(offsets):
    weights = [spline(offsets[axis : axis + 1]) for axis in range(3)]
    slopes = [
        [weights[axis][node] * (float(node) - offsets[axis : axis + 1]) for node in range(3)]
        for axis in range(3)
    ]
    return (weights, slopes)


def rows_iota(count):
    return lax.broadcasted_iota(jnp.int32, (count, 1), 0)


def build(bases, weights, slopes, size_x, size_y, tab, xw, xs, yw, ys):
    width = bases.shape[1]
    from_x = bases[0:1] + 2
    from_y = bases[1:2] + 2
    edge = rows_iota(8)
    for size, start, axis, plain, slope in ((size_x, from_x, 0, xw, xs), (size_y, from_y, 1, yw, ys)):
        place = rows_iota(size) + 2 - start
        plain[0:size] = pick(place, weights[axis])
        slope[0:size] = pick(place, slopes[axis])
        coord = jnp.where(edge < 2, edge, jnp.where(edge < 4, edge + size, OUTSIDE))
        place = coord - start
        plain[size : size + 8] = pick(place, weights[axis])
        slope[size : size + 8] = pick(place, slopes[axis])

    def put(row, count, wx, sx, wy, sy):
        tab[row : row + count, 0:width] = (wx * wy).astype(BF16)
        tab[row : row + count, width : 2 * width] = (sx * wy).astype(BF16)
        tab[row : row + count, 2 * width : 3 * width] = (wx * sy).astype(BF16)

    places, margin = block_rows(size_x, size_y)
    wide_w, wide_s = (xw[0:size_x], xs[0:size_x])
    for k in range(4):
        one = slice(size_y + k, size_y + k + 1)
        put(k * size_x, size_x, wide_w, wide_s, yw[one], ys[one])
    tall_w, tall_s = (yw[0:size_y], ys[0:size_y])
    for k in range(4):
        one = slice(size_x + k, size_x + k + 1)
        put(places[2][0] + k * size_y, size_y, xw[one], xs[one], tall_w, tall_s)
    spot = rows_iota(CORNER_ROWS)
    for k in range(4):
        high_x, high_y = (k // 2, k % 2)
        coord_x = jnp.where(spot < 4, (spot >> 1) + high_x * (size_x + 2), OUTSIDE)
        coord_y = jnp.where(spot < 4, (spot & 1) + high_y * (size_y + 2), OUTSIDE)
        place_x = coord_x - from_x
        place_y = coord_y - from_y
        put(
            places[4 + k][0],
            CORNER_ROWS,
            pick(place_x, weights[0]),
            pick(place_x, slopes[0]),
            pick(place_y, weights[1]),
            pick(place_y, slopes[1]),
        )
    for x in range(size_x):
        one = slice(x, x + 1)
        put(margin + x * size_y, size_y, xw[one], xs[one], tall_w, tall_s)


def depth_tables(bases, weights, slopes, depth):
    place = rows_iota(depth) - bases[2:3]
    return (pick(place, weights[2]), pick(place, slopes[2]))


def scatter_chunk(bases, offsets, vel, aff, vol, sizes, tab, right, tables, total):
    size_x, size_y, depth = sizes
    width = bases.shape[1]
    weights, slopes = weights_of(offsets)
    build(bases, weights, slopes, size_x, size_y, tab, *tables)
    depth_w, depth_s = depth_tables(bases, weights, slopes, depth)
    stress = -STIFFNESS * (vol - 1.0)

    def entry(i, j):
        value = PARTICLE_MASS * aff[3 * i + j]
        return value + stress if i == j else value

    zeros = jnp.zeros((depth, 2 * width), BF16)
    right[0:depth, 0:width] = (depth_w * PARTICLE_MASS).astype(BF16)
    right[0:depth, width : 3 * width] = zeros
    for i in range(3):
        rows = slice((i + 1) * depth, (i + 2) * depth)
        moment = PARTICLE_MASS * vel[i]
        right[rows, 0:width] = (depth_w * moment + depth_s * entry(i, 2)).astype(BF16)
        right[rows, width : 2 * width] = (depth_w * entry(i, 0)).astype(BF16)
        right[rows, 2 * width : 3 * width] = (depth_w * entry(i, 1)).astype(BF16)
    total[...] += lax.dot_general(tab[...], right[...], NT, preferred_element_type=F32)


def gather_chunk(bases, offsets, vol, sizes, wide, tab, result, tables):
    size_x, size_y, depth = sizes
    width = bases.shape[1]
    weights, slopes = weights_of(offsets)
    build(bases, weights, slopes, size_x, size_y, tab, *tables)
    depth_w, depth_s = depth_tables(bases, weights, slopes, depth)
    result[...] = jnp.dot(wide[...], tab[...], preferred_element_type=F32)
    vel, aff = ([], [None] * 9)
    for i in range(3):
        rows = slice(i * depth, (i + 1) * depth)
        plain = result[rows, 0:width]
        vel.append(jnp.sum(plain * depth_w, 0, keepdims=True))
        aff[3 * i + 2] = 4.0 * jnp.sum(plain * depth_s, 0, keepdims=True)
        aff[3 * i] = 4.0 * jnp.sum(result[rows, width : 2 * width] * depth_w, 0, keepdims=True)
        aff[3 * i + 1] = 4.0 * jnp.sum(
            result[rows, 2 * width : 3 * width] * depth_w, 0, keepdims=True
        )
    vol = vol * (1.0 + TIME_STEP * (aff[0] + aff[4] + aff[8]))
    return (vel, aff, vol)


def take_rows(ref, lanes, count):
    return [ref[k : k + 1, lanes] for k in range(count)]


def first_kernel(sizes, chunk, base, offset, vel, aff, vol, core, margins, tab, right, total, *tables):
    total[...] = jnp.zeros_like(total)

    def body(step, carry):
        lanes = pl.ds(pl.multiple_of(step * chunk, chunk), chunk)
        scatter_chunk(
            base[0, :, lanes], offset[0, :, lanes], take_rows(vel, lanes, 3),
            take_rows(aff, lanes, 9), vol[:, lanes], sizes, tab, right, tables, total,
        )
        return carry

    lax.fori_loop(0, vel.shape[1] // chunk, body, 0)
    edge = margins.shape[0]
    margins[...] = total[0:edge].astype(BF16)
    core[...] = total[edge:]


def middle_kernel(sizes, chunk, base, offset, vol, wide, core, margins, vol_out, tab, result, right, total, *tables):
    total[...] = jnp.zeros_like(total)

    def body(step, carry):
        lanes = pl.ds(pl.multiple_of(step * chunk, chunk), chunk)
        vel, aff, ratio = gather_chunk(
            base[0, :, lanes], offset[0, :, lanes], vol[:, lanes], sizes, wide, tab, result, tables
        )
        vol_out[:, lanes] = ratio
        scatter_chunk(
            base[1, :, lanes], offset[1, :, lanes], vel, aff, ratio, sizes, tab, right, tables, total
        )
        return carry

    lax.fori_loop(0, vol.shape[1] // chunk, body, 0)
    edge = margins.shape[0]
    margins[...] = total[0:edge].astype(BF16)
    core[...] = total[edge:]


def last_kernel(sizes, chunk, capacity, counts, base, offset, vol, wide, direction, own, buckets, tab, result, state, slots, *tables):
    size_x, size_y, _ = sizes
    count_x, count_y = counts
    index_x = lax.axis_index("gx")
    index_y = lax.axis_index("gy")
    rows = vol.shape[1]

    def route(code):
        step_x = jnp.where(code < 3, -1, jnp.where(code > 5, 1, 0))
        step_y = code - 3 * step_x - 4
        to_x = step_x + index_x
        to_y = step_y + index_y
        inside = (to_x >= 0) & (to_x < count_x) & (to_y >= 0) & (to_y < count_y)
        return (
            jnp.where(inside, code, 4),
            jnp.where(inside, step_x, 0),
            jnp.where(inside, step_y, 0),
        )

    def body(step, carry):
        lanes = pl.ds(pl.multiple_of(step * chunk, chunk), chunk)
        bases = base[1, :, lanes]
        offsets = offset[1, :, lanes]
        vel, aff, ratio = gather_chunk(
            bases, offsets, vol[:, lanes], sizes, wide, tab, result, tables
        )
        moving, step_x, step_y = route(direction[:, lanes])
        shift = (step_x * size_x, step_y * size_y, None)
        for axis in range(3):
            spot = bases[axis : axis + 1].astype(F32) + offsets[axis : axis + 1]
            spot = spot + TIME_STEP * vel[axis]
            if shift[axis] is not None:
                spot = spot - shift[axis].astype(F32)
            state[axis : axis + 1, lanes] = spot
            state[3 + axis : 4 + axis, lanes] = vel[axis]
        for k in range(9):
            state[6 + k : 7 + k, lanes] = aff[k]
        state[15:16, lanes] = ratio
        own[:, lanes] = jnp.where(moving == 4, state[:, lanes], 0.0)
        return carry

    lax.fori_loop(0, rows // chunk, body, 0)

    parts = rows // LANES
    place = rows_iota(8)
    codes = jnp.where(place < 4, place, place + 1)
    hits = []
    for part in range(parts):
        moving, _, _ = route(direction[:, part * LANES : (part + 1) * LANES])
        hits.append(jnp.where(moving == codes, 1.0, 0.0))
    above = lax.broadcasted_iota(jnp.int32, (LANES, 2 * LANES), 0)
    along = lax.broadcasted_iota(jnp.int32, (LANES, 2 * LANES), 1)
    summer = jnp.where(above <= along, 1.0, 0.0).astype(BF16)
    sums = jnp.dot(jnp.concatenate(hits, 0).astype(BF16), summer, preferred_element_type=F32)
    before = (place * capacity).astype(F32)
    before = jnp.broadcast_to(before, (8, LANES))
    for part in range(parts):
        mine = slice(part * 8, (part + 1) * 8)
        slot = jnp.sum(hits[part] * (sums[mine, 0:LANES] + before), 0, keepdims=True) - 1.0
        slots[:, part * LANES : (part + 1) * LANES] = slot.astype(jnp.int32)
        before = before + sums[mine, LANES:]

    value = state[...]
    high = value.astype(BF16)
    rest = value - high.astype(F32)
    middle = rest.astype(BF16)
    low = (rest - middle.astype(F32)).astype(BF16)
    split = jnp.concatenate([high, middle, low], 0)
    for k in range(8):
        chosen = slots[...] - k * capacity == rows_iota(capacity)
        chosen = jnp.where(chosen, 1.0, 0.0).astype(BF16)
        packed = lax.dot_general(split, chosen, NT, preferred_element_type=F32)
        buckets[k] = packed[0:16] + packed[16:32] + packed[32:48]


def neighbour(counts, dx, dy):
    to_x = lax.axis_index("gx") + dx
    to_y = lax.axis_index("gy") + dy
    exists = (to_x >= 0) & (to_x < counts[0]) & (to_y >= 0) & (to_y < counts[1])
    return (exists, {"gx": to_x, "gy": to_y})


def greet(counts):
    barrier = pltpu.get_barrier_semaphore()
    for dx, dy in BLOCKS:
        exists, where = neighbour(counts, dx, dy)

        @pl.when(exists)
        def _():
            pl.semaphore_signal(
                barrier, inc=1, device_id=where, device_id_type=pl.DeviceIdType.MESH
            )

    peers = 0
    for dx, dy in BLOCKS:
        exists, _ = neighbour(counts, dx, dy)
        peers = peers + exists.astype(jnp.int32)
    pl.semaphore_wait(barrier, peers)


def transfers(counts, sign, views, source, target, send_sems, recv_sems):
    copies = []
    for k, (dx, dy) in enumerate(BLOCKS):
        exists, where = neighbour(counts, sign * dx, sign * dy)
        copy = pltpu.make_async_remote_copy(
            src_ref=views(source, k),
            dst_ref=views(target, k),
            send_sem=send_sems.at[k],
            recv_sem=recv_sems.at[k],
            device_id=where,
            device_id_type=pl.DeviceIdType.MESH,
        )
        comes, _ = neighbour(counts, -sign * dx, -sign * dy)
        copies.append((exists, comes, copy))
    return copies


def start_all(copies, views, target):
    for exists, _, copy in copies:
        pl.when(exists)(copy.start)
    for k, (_, comes, _) in enumerate(copies):

        @pl.when(jnp.logical_not(comes))
        def _():
            view = views(target, k)
            view[...] = jnp.zeros(view.shape, view.dtype)


def wait_all(copies):
    for exists, comes, copy in copies:
        pl.when(comes)(copy.wait_recv)
    for exists, comes, copy in copies:
        pl.when(exists)(copy.wait_send)


def grid_kernel(sizes, counts, core, margins, mask, place_in, take_out, wide, got, sent, halo, speed, sends, recvs, sends_b, recvs_b):
    size_x, size_y, depth = sizes
    places, edge = block_rows(size_x, size_y)

    def views(ref, k):
        return ref.at[pl.ds(places[k][0], places[k][1])]

    greet(counts)
    copies = transfers(counts, 1, views, margins, got, sends, recvs)
    start_all(copies, views, got)
    wait_all(copies)
    total = core[...] + jnp.dot(place_in[...], got[...], preferred_element_type=F32)
    mass = jnp.maximum(total[:, 0:depth], MASS_FLOOR)
    keep = (1 - mask[...]).astype(F32)
    for axis in range(3):
        value = total[:, (axis + 1) * depth : (axis + 2) * depth] / mass
        if axis == 2:
            value = value - TIME_STEP * GRAVITY
        speed[:, axis * depth : (axis + 1) * depth] = (value * keep).astype(BF16)
    sent[...] = jnp.dot(take_out[...], speed[...], preferred_element_type=F32).astype(BF16)
    copies = transfers(counts, -1, views, sent, halo, sends_b, recvs_b)
    start_all(copies, views, halo)
    for axis in range(3):
        lanes = slice(axis * depth, (axis + 1) * depth)
        wide[lanes, edge:] = speed[:, lanes].astype(F32).T.astype(BF16)
    wait_all(copies)
    for axis in range(3):
        lanes = slice(axis * depth, (axis + 1) * depth)
        wide[lanes, 0:edge] = halo[:, lanes].astype(F32).T.astype(BF16)


def migrate_kernel(counts, buckets, out, got, sends, recvs):
    capacity = buckets.shape[2]
    order = [0, 1, 2, 3, 5, 6, 7, 8]
    slot_of = [order.index(3 * (dx + 1) + dy + 1) for dx, dy in BLOCKS]

    def views(ref, k):
        return ref.at[slot_of[k]]

    greet(counts)
    copies = transfers(counts, 1, views, buckets, got, sends, recvs)
    start_all(copies, views, got)
    wait_all(copies)
    for k in range(8):
        out[:, k * capacity : (k + 1) * capacity] = got[k]


def vmem(count):
    return [pl.BlockSpec(memory_space=pltpu.VMEM)] * count


def per_device(counts, base, offset, velocity, affine, volume, node_mask, direction):
    sizes = node_mask.shape
    size_x, size_y, depth = sizes
    rows = velocity.shape[1]
    capacity = rows // 16
    chunk = min(rows, 512)
    _, edge = block_rows(size_x, size_y)
    cells = size_x * size_y
    all_rows = edge + cells
    volume = volume.reshape(1, rows)
    direction = direction.reshape(1, rows)
    mask = node_mask.reshape(cells, depth)
    owners = owner_rows(size_x, size_y)
    choose = (owners[:, None] == np.arange(cells)[None]).astype(np.float32)
    take_out = jnp.asarray(choose, BF16)
    place_in = jnp.asarray(choose.T, BF16)

    tab = pltpu.VMEM((all_rows, 3 * chunk), BF16)
    right = pltpu.VMEM((4 * depth, 3 * chunk), BF16)
    result = pltpu.VMEM((3 * depth, 3 * chunk), F32)
    total = pltpu.VMEM((all_rows, 4 * depth), F32)
    tables = [pltpu.VMEM((size_x + 8, chunk), F32)] * 2 + [pltpu.VMEM((size_y + 8, chunk), F32)] * 2
    grid_out = [
        jax.ShapeDtypeStruct((cells, 4 * depth), F32),
        jax.ShapeDtypeStruct((edge, 4 * depth), BF16),
    ]
    params = pltpu.CompilerParams(vmem_limit_bytes=56 * 1024 * 1024)

    core, margins = pl.pallas_call(
        functools.partial(first_kernel, sizes, chunk),
        out_shape=grid_out,
        in_specs=vmem(5),
        out_specs=vmem(2),
        scratch_shapes=[tab, right, total] + tables,
        compiler_params=params,
        name="scatter",
    )(base, offset, velocity, affine, volume)

    def exchange(core, margins):
        return pl.pallas_call(
            functools.partial(grid_kernel, sizes, counts),
            out_shape=jax.ShapeDtypeStruct((3 * depth, all_rows), BF16),
            in_specs=vmem(5),
            out_specs=vmem(1)[0],
            scratch_shapes=[
                pltpu.VMEM((edge, 4 * depth), BF16),
                pltpu.VMEM((edge, 3 * depth), BF16),
                pltpu.VMEM((edge, 3 * depth), BF16),
                pltpu.VMEM((cells, 3 * depth), BF16),
            ]
            + [pltpu.SemaphoreType.DMA((8,))] * 4,
            compiler_params=pltpu.CompilerParams(
                collective_id=0, has_side_effects=True, vmem_limit_bytes=56 * 1024 * 1024
            ),
            name="exchange",
        )(core, margins, mask, place_in, take_out)

    wide = exchange(core, margins)
    core, margins, volume = pl.pallas_call(
        functools.partial(middle_kernel, sizes, chunk),
        out_shape=grid_out + [jax.ShapeDtypeStruct((1, rows), F32)],
        in_specs=vmem(4),
        out_specs=vmem(3),
        scratch_shapes=[tab, result, right, total] + tables,
        compiler_params=params,
        name="gather_scatter",
    )(base, offset, volume, wide)
    wide = exchange(core, margins)
    own, buckets = pl.pallas_call(
        functools.partial(last_kernel, sizes, chunk, capacity, counts),
        out_shape=[
            jax.ShapeDtypeStruct((16, rows), F32),
            jax.ShapeDtypeStruct((8, 16, capacity), F32),
        ],
        in_specs=vmem(5),
        out_specs=vmem(2),
        scratch_shapes=[tab, result, pltpu.VMEM((16, rows), F32), pltpu.VMEM((1, rows), jnp.int32)]
        + tables,
        compiler_params=params,
        name="gather_pack",
    )(base, offset, volume, wide, direction)
    arrived = pl.pallas_call(
        functools.partial(migrate_kernel, counts),
        out_shape=jax.ShapeDtypeStruct((16, 8 * capacity), F32),
        in_specs=vmem(1),
        out_specs=vmem(1)[0],
        scratch_shapes=[pltpu.VMEM((8, 16, capacity), F32)] + [pltpu.SemaphoreType.DMA((8,))] * 2,
        compiler_params=pltpu.CompilerParams(collective_id=1, has_side_effects=True),
        name="migrate",
    )(buckets)
    return jnp.concatenate([own, arrived], 1)


def solution(mesh):
    counts = (mesh.shape["gx"], mesh.shape["gy"])
    placed = (
        P(None, None, ("gx", "gy")),
        P(None, None, ("gx", "gy")),
        P(None, ("gx", "gy")),
        P(None, ("gx", "gy")),
        P(("gx", "gy")),
        P("gx", "gy", None),
        P(("gx", "gy")),
    )
    return jax.shard_map(
        functools.partial(per_device, counts),
        mesh=mesh,
        in_specs=placed,
        out_specs=P(None, ("gx", "gy")),
        check_vma=False,
    )
```

```python
import functools

import jax
import jax.numpy as jnp
import numpy as np
from jax import lax
from jax.experimental import pallas as pl
from jax.experimental.pallas import tpu as pltpu
from jax.sharding import PartitionSpec as P

PARTICLE_MASS = 1.0
STIFFNESS = 4.0
TIME_STEP = 0.1
GRAVITY = 3.0
MASS_FLOOR = 0.5
LANES = 128
OUTSIDE = -100

F32 = jnp.float32
BF16 = jnp.bfloat16
NT = (((1,), (1,)), ((), ()))

BLOCKS = ((0, -1), (0, 1), (-1, 0), (1, 0), (-1, -1), (-1, 1), (1, -1), (1, 1))
CORNER_ROWS = 16


def block_rows(size_x, size_y):
    counts = [2 * size_x] * 2 + [2 * size_y] * 2 + [CORNER_ROWS] * 4
    starts = [sum(counts[:place]) for place in range(8)]
    return (list(zip(starts, counts)), sum(counts))


def owner_rows(size_x, size_y):
    places, total = block_rows(size_x, size_y)
    rows = np.full(total, -1, np.int64)
    for (dx, dy), (start, _) in zip(BLOCKS, places):
        span_x = range(2) if dx else range(size_x)
        span_y = range(2) if dy else range(size_y)
        low_x = size_x - 2 if dx < 0 else 0
        low_y = size_y - 2 if dy < 0 else 0
        for x in span_x:
            for y in span_y:
                if dx and dy:
                    spot = 2 * x + y
                elif dx:
                    spot = x * size_y + y
                else:
                    spot = y * size_x + x
                rows[start + spot] = (low_x + x) * size_y + low_y + y
    return rows


def spline(frac):
    return [0.5 * (1.5 - frac) ** 2, 0.75 - (frac - 1.0) ** 2, 0.5 * (frac - 0.5) ** 2]


def pick(place, values):
    return jnp.where(
        place == 0,
        values[0],
        jnp.where(place == 1, values[1], jnp.where(place == 2, values[2], 0.0)),
    )


def weights_of(offsets):
    weights = [spline(offsets[axis : axis + 1]) for axis in range(3)]
    slopes = [
        [weights[axis][node] * (float(node) - offsets[axis : axis + 1]) for node in range(3)]
        for axis in range(3)
    ]
    return (weights, slopes)


def rows_iota(count):
    return lax.broadcasted_iota(jnp.int32, (count, 1), 0)


def build(bases, weights, slopes, size_x, size_y, tab, xw, xs, yw, ys):
    width = bases.shape[1]
    from_x = bases[0:1] + 2
    from_y = bases[1:2] + 2
    edge = rows_iota(8)
    for size, start, axis, plain, slope in ((size_x, from_x, 0, xw, xs), (size_y, from_y, 1, yw, ys)):
        place = rows_iota(size) + 2 - start
        plain[0:size] = pick(place, weights[axis])
        slope[0:size] = pick(place, slopes[axis])
        coord = jnp.where(edge < 2, edge, jnp.where(edge < 4, edge + size, OUTSIDE))
        place = coord - start
        plain[size : size + 8] = pick(place, weights[axis])
        slope[size : size + 8] = pick(place, slopes[axis])

    def put(row, count, wx, sx, wy, sy):
        tab[row : row + count, 0:width] = (wx * wy).astype(BF16)
        tab[row : row + count, width : 2 * width] = (sx * wy).astype(BF16)
        tab[row : row + count, 2 * width : 3 * width] = (wx * sy).astype(BF16)

    places, margin = block_rows(size_x, size_y)
    wide_w, wide_s = (xw[0:size_x], xs[0:size_x])
    for k in range(4):
        one = slice(size_y + k, size_y + k + 1)
        put(k * size_x, size_x, wide_w, wide_s, yw[one], ys[one])
    tall_w, tall_s = (yw[0:size_y], ys[0:size_y])
    for k in range(4):
        one = slice(size_x + k, size_x + k + 1)
        put(places[2][0] + k * size_y, size_y, xw[one], xs[one], tall_w, tall_s)
    spot = rows_iota(CORNER_ROWS)
    for k in range(4):
        high_x, high_y = (k // 2, k % 2)
        coord_x = jnp.where(spot < 4, (spot >> 1) + high_x * (size_x + 2), OUTSIDE)
        coord_y = jnp.where(spot < 4, (spot & 1) + high_y * (size_y + 2), OUTSIDE)
        place_x = coord_x - from_x
        place_y = coord_y - from_y
        put(
            places[4 + k][0],
            CORNER_ROWS,
            pick(place_x, weights[0]),
            pick(place_x, slopes[0]),
            pick(place_y, weights[1]),
            pick(place_y, slopes[1]),
        )
    for x in range(size_x):
        one = slice(x, x + 1)
        put(margin + x * size_y, size_y, xw[one], xs[one], tall_w, tall_s)


def depth_tables(bases, weights, slopes, depth):
    place = rows_iota(depth) - bases[2:3]
    return (pick(place, weights[2]), pick(place, slopes[2]))


def scatter_chunk(bases, offsets, vel, aff, vol, sizes, tab, right, tables, total):
    size_x, size_y, depth = sizes
    _, edge = block_rows(size_x, size_y)
    width = bases.shape[1]
    weights, slopes = weights_of(offsets)
    build(bases, weights, slopes, size_x, size_y, tab, *tables)
    depth_w, depth_s = depth_tables(bases, weights, slopes, depth)
    stress = -STIFFNESS * (vol - 1.0)

    def entry(i, j):
        value = PARTICLE_MASS * aff[3 * i + j]
        return value + stress if i == j else value

    zeros = jnp.zeros((depth, 2 * width), BF16)
    right[0:depth, 0:width] = (depth_w * PARTICLE_MASS).astype(BF16)
    right[0:depth, width : 3 * width] = zeros
    for i in range(3):
        rows = slice((i + 1) * depth, (i + 2) * depth)
        moment = PARTICLE_MASS * vel[i]
        right[rows, 0:width] = (depth_w * moment + depth_s * entry(i, 2)).astype(BF16)
        right[rows, width : 2 * width] = (depth_w * entry(i, 0)).astype(BF16)
        right[rows, 2 * width : 3 * width] = (depth_w * entry(i, 1)).astype(BF16)
    total[0:edge] += lax.dot_general(tab[0:edge], right[...], NT, preferred_element_type=F32)


def gather_chunk(bases, offsets, vol, sizes, wide, tab, result, tables):
    size_x, size_y, depth = sizes
    width = bases.shape[1]
    weights, slopes = weights_of(offsets)
    build(bases, weights, slopes, size_x, size_y, tab, *tables)
    depth_w, depth_s = depth_tables(bases, weights, slopes, depth)
    result[...] = jnp.dot(wide[...], tab[...], preferred_element_type=F32)
    vel, aff = ([], [None] * 9)
    for i in range(3):
        rows = slice(i * depth, (i + 1) * depth)
        plain = result[rows, 0:width]
        vel.append(jnp.sum(plain * depth_w, 0, keepdims=True))
        aff[3 * i + 2] = 4.0 * jnp.sum(plain * depth_s, 0, keepdims=True)
        aff[3 * i] = 4.0 * jnp.sum(result[rows, width : 2 * width] * depth_w, 0, keepdims=True)
        aff[3 * i + 1] = 4.0 * jnp.sum(
            result[rows, 2 * width : 3 * width] * depth_w, 0, keepdims=True
        )
    vol = vol * (1.0 + TIME_STEP * (aff[0] + aff[4] + aff[8]))
    return (vel, aff, vol)


def take_rows(ref, lanes, count):
    return [ref[k : k + 1, lanes] for k in range(count)]


def first_kernel(sizes, counts, chunk, base, offset, vel, aff, vol, mask, place_in, take_out, wide, tab, right, total, xw, xs, yw, ys, *remote):
    greet(counts)
    total[...] = jnp.zeros_like(total)

    def body(step, carry):
        lanes = pl.ds(pl.multiple_of(step * chunk, chunk), chunk)
        scatter_chunk(
            base[0, :, lanes], offset[0, :, lanes], take_rows(vel, lanes, 3),
            take_rows(aff, lanes, 9), vol[:, lanes], sizes, tab.at[step], right.at[step],
            (xw, xs, yw, ys), total,
        )
        return carry

    lax.fori_loop(0, vel.shape[1] // chunk, body, 0)
    exchange(sizes, counts, mask, place_in, take_out, wide, tab, right, total, *remote)


def middle_kernel(sizes, counts, chunk, base, offset, vol, before, mask, place_in, take_out, wide, vol_out, seen, result, tab, right, total, xw, xs, yw, ys, *remote):
    greet(counts)
    total[...] = jnp.zeros_like(total)

    def body(step, carry):
        lanes = pl.ds(pl.multiple_of(step * chunk, chunk), chunk)
        vel, aff, ratio = gather_chunk(
            base[0, :, lanes], offset[0, :, lanes], vol[:, lanes], sizes, before, seen, result,
            (xw, xs, yw, ys),
        )
        vol_out[:, lanes] = ratio
        scatter_chunk(
            base[1, :, lanes], offset[1, :, lanes], vel, aff, ratio, sizes, tab.at[step],
            right.at[step], (xw, xs, yw, ys), total,
        )
        return carry

    lax.fori_loop(0, vol.shape[1] // chunk, body, 0)
    exchange(sizes, counts, mask, place_in, take_out, wide, tab, right, total, *remote)


def last_kernel(sizes, chunk, capacity, counts, base, offset, vol, wide, direction, out, tab, result, state, slots, xw, xs, yw, ys, buckets, got, sends, recvs):
    greet(counts)
    tables = (xw, xs, yw, ys)
    size_x, size_y, _ = sizes
    count_x, count_y = counts
    index_x = lax.axis_index("gx")
    index_y = lax.axis_index("gy")
    rows = vol.shape[1]

    def route(code):
        step_x = jnp.where(code < 3, -1, jnp.where(code > 5, 1, 0))
        step_y = code - 3 * step_x - 4
        to_x = step_x + index_x
        to_y = step_y + index_y
        inside = (to_x >= 0) & (to_x < count_x) & (to_y >= 0) & (to_y < count_y)
        return (
            jnp.where(inside, code, 4),
            jnp.where(inside, step_x, 0),
            jnp.where(inside, step_y, 0),
        )

    def body(step, carry):
        lanes = pl.ds(pl.multiple_of(step * chunk, chunk), chunk)
        bases = base[1, :, lanes]
        offsets = offset[1, :, lanes]
        vel, aff, ratio = gather_chunk(
            bases, offsets, vol[:, lanes], sizes, wide, tab, result, tables
        )
        moving, step_x, step_y = route(direction[:, lanes])
        shift = (step_x * size_x, step_y * size_y, None)
        for axis in range(3):
            spot = bases[axis : axis + 1].astype(F32) + offsets[axis : axis + 1]
            spot = spot + TIME_STEP * vel[axis]
            if shift[axis] is not None:
                spot = spot - shift[axis].astype(F32)
            state[axis : axis + 1, lanes] = spot
            state[3 + axis : 4 + axis, lanes] = vel[axis]
        for k in range(9):
            state[6 + k : 7 + k, lanes] = aff[k]
        state[15:16, lanes] = ratio
        out[:, lanes] = jnp.where(moving == 4, state[:, lanes], 0.0)
        return carry

    lax.fori_loop(0, rows // chunk, body, 0)

    parts = rows // LANES
    place = rows_iota(8)
    codes = jnp.where(place < 4, place, place + 1)
    hits = []
    for part in range(parts):
        moving, _, _ = route(direction[:, part * LANES : (part + 1) * LANES])
        hits.append(jnp.where(moving == codes, 1.0, 0.0))
    above = lax.broadcasted_iota(jnp.int32, (LANES, 2 * LANES), 0)
    along = lax.broadcasted_iota(jnp.int32, (LANES, 2 * LANES), 1)
    summer = jnp.where(above <= along, 1.0, 0.0).astype(BF16)
    sums = jnp.dot(jnp.concatenate(hits, 0).astype(BF16), summer, preferred_element_type=F32)
    before = (place * capacity).astype(F32)
    before = jnp.broadcast_to(before, (8, LANES))
    for part in range(parts):
        mine = slice(part * 8, (part + 1) * 8)
        slot = jnp.sum(hits[part] * (sums[mine, 0:LANES] + before), 0, keepdims=True) - 1.0
        slots[:, part * LANES : (part + 1) * LANES] = slot.astype(jnp.int32)
        before = before + sums[mine, LANES:]

    value = state[...]
    high = value.astype(BF16)
    rest = value - high.astype(F32)
    middle = rest.astype(BF16)
    low = (rest - middle.astype(F32)).astype(BF16)
    split = jnp.concatenate([high, middle, low], 0)
    for k in range(8):
        chosen = slots[...] - k * capacity == rows_iota(capacity)
        chosen = jnp.where(chosen, 1.0, 0.0).astype(BF16)
        packed = lax.dot_general(split, chosen, NT, preferred_element_type=F32)
        buckets[k] = packed[0:16] + packed[16:32] + packed[32:48]
    migrate(counts, buckets, out, got, sends, recvs)


def neighbour(counts, dx, dy):
    to_x = lax.axis_index("gx") + dx
    to_y = lax.axis_index("gy") + dy
    exists = (to_x >= 0) & (to_x < counts[0]) & (to_y >= 0) & (to_y < counts[1])
    return (exists, {"gx": to_x, "gy": to_y})


def greet(counts):
    barrier = pltpu.get_barrier_semaphore()
    for dx, dy in BLOCKS:
        exists, where = neighbour(counts, dx, dy)

        @pl.when(exists)
        def _():
            pl.semaphore_signal(
                barrier, inc=1, device_id=where, device_id_type=pl.DeviceIdType.MESH
            )


def await_peers(counts):
    barrier = pltpu.get_barrier_semaphore()
    peers = 0
    for dx, dy in BLOCKS:
        exists, _ = neighbour(counts, dx, dy)
        peers = peers + exists.astype(jnp.int32)
    pl.semaphore_wait(barrier, peers)


def transfers(counts, sign, source, target, send_sems, recv_sems):
    copies = []
    for k, (dx, dy) in enumerate(BLOCKS):
        exists, where = neighbour(counts, sign * dx, sign * dy)
        copy = pltpu.make_async_remote_copy(
            src_ref=source(k),
            dst_ref=target(k),
            send_sem=send_sems.at[k],
            recv_sem=recv_sems.at[k],
            device_id=where,
            device_id_type=pl.DeviceIdType.MESH,
        )
        comes, _ = neighbour(counts, -sign * dx, -sign * dy)
        copies.append((exists, comes, copy))
    return copies


def start_all(copies, target):
    for exists, _, copy in copies:
        pl.when(exists)(copy.start)
    for k, (_, comes, _) in enumerate(copies):

        @pl.when(jnp.logical_not(comes))
        def _():
            view = target(k)
            view[...] = jnp.zeros(view.shape, view.dtype)


def wait_all(copies):
    for _, comes, copy in copies:
        pl.when(comes)(copy.wait_recv)
    for exists, _, copy in copies:
        pl.when(exists)(copy.wait_send)


def pack_corners(value, channels, depth, spread):
    for k in range(4):
        for c in range(channels):
            spread[k * CORNER_ROWS + 4 * c : k * CORNER_ROWS + 4 * c + 4, :] = value(
                slice(k * CORNER_ROWS, k * CORNER_ROWS + 4), slice(c * depth, (c + 1) * depth)
            )


def unpack_corners(spread, channels, depth, square):
    square[...] = jnp.zeros_like(square)
    for k in range(4):
        for c in range(channels):
            square[
                k * CORNER_ROWS : k * CORNER_ROWS + 4, c * depth : (c + 1) * depth
            ] = spread[k * CORNER_ROWS + 4 * c : k * CORNER_ROWS + 4 * c + 4, :]


def exchange(sizes, counts, mask, place_in, take_out, wide, tab, right, total, margins, corners, got, got_corners, sent, sent_corners, halo, halo_corners, spread, square, speed, drawn, sends, recvs, sends_b, recvs_b):
    size_x, size_y, depth = sizes
    places, edge = block_rows(size_x, size_y)
    inner = places[4][0]

    def views(sides, tiles):
        def view(k):
            if k < 4:
                return sides.at[pl.ds(places[k][0], places[k][1])]
            return tiles.at[pl.ds((k - 4) * CORNER_ROWS, CORNER_ROWS)]

        return view

    margins[...] = total[0:inner].astype(BF16)

    def corner_of(rows, lanes):
        return total[inner + rows.start : inner + rows.stop, lanes]

    pack_corners(corner_of, 4, depth, spread)
    corners[...] = spread[...].astype(BF16)
    await_peers(counts)
    arriving = views(got, got_corners)
    copies = transfers(counts, 1, views(margins, corners), arriving, sends, recvs)
    start_all(copies, arriving)

    def body(step, carry):
        total[edge:] += lax.dot_general(
            tab[step, edge:], right[step], NT, preferred_element_type=F32
        )
        return carry

    lax.fori_loop(0, tab.shape[0], body, 0)
    wait_all(copies)
    spread[...] = got_corners[...].astype(F32)
    unpack_corners(spread, 4, depth, square)
    received = jnp.concatenate([got[...], square[...].astype(BF16)], 0)
    full = total[edge:] + jnp.dot(place_in[...], received, preferred_element_type=F32)
    mass = jnp.maximum(full[:, 0:depth], MASS_FLOOR)
    keep = (1 - mask[...]).astype(F32)
    for axis in range(3):
        value = full[:, (axis + 1) * depth : (axis + 2) * depth] / mass
        if axis == 2:
            value = value - TIME_STEP * GRAVITY
        speed[:, axis * depth : (axis + 1) * depth] = (value * keep).astype(BF16)
    drawn[...] = jnp.dot(take_out[...], speed[...], preferred_element_type=F32)
    sent[...] = drawn[0:inner].astype(BF16)

    def drawn_corner(rows, lanes):
        return drawn[inner + rows.start : inner + rows.stop, lanes]

    pack_corners(drawn_corner, 3, depth, spread)
    sent_corners[...] = spread[...].astype(BF16)
    arriving = views(halo, halo_corners)
    copies = transfers(counts, -1, views(sent, sent_corners), arriving, sends_b, recvs_b)
    start_all(copies, arriving)
    for axis in range(3):
        lanes = slice(axis * depth, (axis + 1) * depth)
        wide[lanes, edge:] = speed[:, lanes].astype(F32).T.astype(BF16)
    wait_all(copies)
    spread[...] = halo_corners[...].astype(F32)
    unpack_corners(spread, 3, depth, square)
    for axis in range(3):
        lanes = slice(axis * depth, (axis + 1) * depth)
        outer = jnp.concatenate([halo[:, lanes].astype(F32), square[:, lanes]], 0)
        wide[lanes, 0:edge] = outer.T.astype(BF16)


def migrate(counts, buckets, out, got, sends, recvs):
    capacity = buckets.shape[2]
    rows = out.shape[1] - 8 * capacity
    order = [0, 1, 2, 3, 5, 6, 7, 8]
    slot_of = [order.index(3 * (dx + 1) + dy + 1) for dx, dy in BLOCKS]

    def views(ref):
        return lambda k: ref.at[slot_of[k]]

    await_peers(counts)
    copies = transfers(counts, 1, views(buckets), views(got), sends, recvs)
    start_all(copies, views(got))
    wait_all(copies)
    for k in range(8):
        out[:, rows + k * capacity : rows + (k + 1) * capacity] = got[k]


def vmem(count):
    return [pl.BlockSpec(memory_space=pltpu.VMEM)] * count


def per_device(counts, base, offset, velocity, affine, volume, node_mask, direction):
    sizes = node_mask.shape
    size_x, size_y, depth = sizes
    rows = velocity.shape[1]
    capacity = rows // 16
    chunk = min(rows, 512)
    _, edge = block_rows(size_x, size_y)
    cells = size_x * size_y
    all_rows = edge + cells
    volume = volume.reshape(1, rows)
    direction = direction.reshape(1, rows)
    mask = node_mask.reshape(cells, depth)
    owners = owner_rows(size_x, size_y)
    choose = (owners[:, None] == np.arange(cells)[None]).astype(np.float32)
    take_out = jnp.asarray(choose, BF16)
    place_in = jnp.asarray(choose.T, BF16)

    inner = edge - 4 * CORNER_ROWS
    steps = rows // chunk
    seen = pltpu.VMEM((all_rows, 3 * chunk), BF16)
    result = pltpu.VMEM((3 * depth, 3 * chunk), F32)
    tables = [pltpu.VMEM((size_x + 8, chunk), F32)] * 2 + [pltpu.VMEM((size_y + 8, chunk), F32)] * 2
    spread = [
        pltpu.VMEM((steps, all_rows, 3 * chunk), BF16),
        pltpu.VMEM((steps, 4 * depth, 3 * chunk), BF16),
        pltpu.VMEM((all_rows, 4 * depth), F32),
    ] + tables
    remote = [
        pltpu.VMEM((inner, 4 * depth), BF16),
        pltpu.VMEM((4 * CORNER_ROWS, depth), BF16),
        pltpu.VMEM((inner, 4 * depth), BF16),
        pltpu.VMEM((4 * CORNER_ROWS, depth), BF16),
        pltpu.VMEM((inner, 3 * depth), BF16),
        pltpu.VMEM((4 * CORNER_ROWS, depth), BF16),
        pltpu.VMEM((inner, 3 * depth), BF16),
        pltpu.VMEM((4 * CORNER_ROWS, depth), BF16),
        pltpu.VMEM((4 * CORNER_ROWS, depth), F32),
        pltpu.VMEM((4 * CORNER_ROWS, 4 * depth), F32),
        pltpu.VMEM((cells, 3 * depth), BF16),
        pltpu.VMEM((edge, 3 * depth), F32),
    ] + [pltpu.SemaphoreType.DMA((8,))] * 4
    wide_out = jax.ShapeDtypeStruct((3 * depth, all_rows), BF16)

    def params(number):
        return pltpu.CompilerParams(
            collective_id=number, has_side_effects=True, vmem_limit_bytes=56 * 1024 * 1024
        )

    wide = pl.pallas_call(
        functools.partial(first_kernel, sizes, counts, chunk),
        out_shape=wide_out,
        in_specs=vmem(8),
        out_specs=vmem(1)[0],
        scratch_shapes=spread + remote,
        compiler_params=params(0),
        name="scatter",
    )(base, offset, velocity, affine, volume, mask, place_in, take_out)
    wide, volume = pl.pallas_call(
        functools.partial(middle_kernel, sizes, counts, chunk),
        out_shape=[wide_out, jax.ShapeDtypeStruct((1, rows), F32)],
        in_specs=vmem(7),
        out_specs=vmem(2),
        scratch_shapes=[seen, result] + spread + remote,
        compiler_params=params(1),
        name="gather_scatter",
    )(base, offset, volume, wide, mask, place_in, take_out)
    return pl.pallas_call(
        functools.partial(last_kernel, sizes, chunk, capacity, counts),
        out_shape=jax.ShapeDtypeStruct((16, rows + 8 * capacity), F32),
        in_specs=vmem(5),
        out_specs=vmem(1)[0],
        scratch_shapes=[seen, result, pltpu.VMEM((16, rows), F32), pltpu.VMEM((1, rows), jnp.int32)]
        + tables
        + [pltpu.VMEM((8, 16, capacity), F32)] * 2
        + [pltpu.SemaphoreType.DMA((8,))] * 2,
        compiler_params=params(2),
        name="gather_pack",
    )(base, offset, volume, wide, direction)


def solution(mesh):
    counts = (mesh.shape["gx"], mesh.shape["gy"])
    placed = (
        P(None, None, ("gx", "gy")),
        P(None, None, ("gx", "gy")),
        P(None, ("gx", "gy")),
        P(None, ("gx", "gy")),
        P(("gx", "gy")),
        P("gx", "gy", None),
        P(("gx", "gy")),
    )
    return jax.shard_map(
        functools.partial(per_device, counts),
        mesh=mesh,
        in_specs=placed,
        out_specs=P(None, ("gx", "gy")),
        check_vma=False,
    )
```

```python
import functools

import jax
import jax.numpy as jnp
import numpy as np
from jax import lax
from jax.experimental import pallas as pl
from jax.experimental.pallas import tpu as pltpu
from jax.sharding import PartitionSpec as P

PARTICLE_MASS = 1.0
STIFFNESS = 4.0
TIME_STEP = 0.1
GRAVITY = 3.0
MASS_FLOOR = 0.5
LANES = 128
OUTSIDE = -100

F32 = jnp.float32
BF16 = jnp.bfloat16
NT = (((1,), (1,)), ((), ()))

BLOCKS = ((0, -1), (0, 1), (-1, 0), (1, 0), (-1, -1), (-1, 1), (1, -1), (1, 1))
CORNER_ROWS = 16


def block_rows(size_x, size_y):
    counts = [2 * size_x] * 2 + [2 * size_y] * 2 + [CORNER_ROWS] * 4
    starts = [sum(counts[:place]) for place in range(8)]
    return (list(zip(starts, counts)), sum(counts))


def owner_rows(size_x, size_y):
    places, total = block_rows(size_x, size_y)
    rows = np.full(total, -1, np.int64)
    for (dx, dy), (start, _) in zip(BLOCKS, places):
        span_x = range(2) if dx else range(size_x)
        span_y = range(2) if dy else range(size_y)
        low_x = size_x - 2 if dx < 0 else 0
        low_y = size_y - 2 if dy < 0 else 0
        for x in span_x:
            for y in span_y:
                if dx and dy:
                    spot = 2 * x + y
                elif dx:
                    spot = x * size_y + y
                else:
                    spot = y * size_x + x
                rows[start + spot] = (low_x + x) * size_y + low_y + y
    return rows


def spline(frac):
    return [0.5 * (1.5 - frac) ** 2, 0.75 - (frac - 1.0) ** 2, 0.5 * (frac - 0.5) ** 2]


def pick(place, values):
    return jnp.where(
        place == 0,
        values[0],
        jnp.where(place == 1, values[1], jnp.where(place == 2, values[2], 0.0)),
    )


def weights_of(offsets):
    weights = [spline(offsets[axis : axis + 1]) for axis in range(3)]
    slopes = [
        [weights[axis][node] * (float(node) - offsets[axis : axis + 1]) for node in range(3)]
        for axis in range(3)
    ]
    return (weights, slopes)


def rows_iota(count):
    return lax.broadcasted_iota(jnp.int32, (count, 1), 0)


def build(bases, weights, slopes, size_x, size_y, tab, xw, xs, yw, ys):
    width = bases.shape[1]
    from_x = bases[0:1] + 2
    from_y = bases[1:2] + 2
    edge = rows_iota(8)
    for size, start, axis, plain, slope in ((size_x, from_x, 0, xw, xs), (size_y, from_y, 1, yw, ys)):
        place = rows_iota(size) + 2 - start
        plain[0:size] = pick(place, weights[axis])
        slope[0:size] = pick(place, slopes[axis])
        coord = jnp.where(edge < 2, edge, jnp.where(edge < 4, edge + size, OUTSIDE))
        place = coord - start
        plain[size : size + 8] = pick(place, weights[axis])
        slope[size : size + 8] = pick(place, slopes[axis])

    def put(row, count, wx, sx, wy, sy):
        tab[row : row + count, 0:width] = (wx * wy).astype(BF16)
        tab[row : row + count, width : 2 * width] = (sx * wy).astype(BF16)
        tab[row : row + count, 2 * width : 3 * width] = (wx * sy).astype(BF16)

    places, margin = block_rows(size_x, size_y)
    wide_w, wide_s = (xw[0:size_x], xs[0:size_x])
    for k in range(4):
        one = slice(size_y + k, size_y + k + 1)
        put(k * size_x, size_x, wide_w, wide_s, yw[one], ys[one])
    tall_w, tall_s = (yw[0:size_y], ys[0:size_y])
    for k in range(4):
        one = slice(size_x + k, size_x + k + 1)
        put(places[2][0] + k * size_y, size_y, xw[one], xs[one], tall_w, tall_s)
    spot = rows_iota(CORNER_ROWS)
    for k in range(4):
        high_x, high_y = (k // 2, k % 2)
        coord_x = jnp.where(spot < 4, (spot >> 1) + high_x * (size_x + 2), OUTSIDE)
        coord_y = jnp.where(spot < 4, (spot & 1) + high_y * (size_y + 2), OUTSIDE)
        place_x = coord_x - from_x
        place_y = coord_y - from_y
        put(
            places[4 + k][0],
            CORNER_ROWS,
            pick(place_x, weights[0]),
            pick(place_x, slopes[0]),
            pick(place_y, weights[1]),
            pick(place_y, slopes[1]),
        )
    for x in range(size_x):
        one = slice(x, x + 1)
        put(margin + x * size_y, size_y, xw[one], xs[one], tall_w, tall_s)


def depth_tables(bases, weights, slopes, depth):
    place = rows_iota(depth) - bases[2:3]
    return (pick(place, weights[2]), pick(place, slopes[2]))


def scatter_chunk(bases, offsets, vel, aff, vol, sizes, tab, right, tables, total):
    size_x, size_y, depth = sizes
    _, edge = block_rows(size_x, size_y)
    width = bases.shape[1]
    weights, slopes = weights_of(offsets)
    build(bases, weights, slopes, size_x, size_y, tab, *tables)
    depth_w, depth_s = depth_tables(bases, weights, slopes, depth)
    stress = -STIFFNESS * (vol - 1.0)

    def entry(i, j):
        value = PARTICLE_MASS * aff[3 * i + j]
        return value + stress if i == j else value

    zeros = jnp.zeros((depth, 2 * width), BF16)
    right[0:depth, 0:width] = (depth_w * PARTICLE_MASS).astype(BF16)
    right[0:depth, width : 3 * width] = zeros
    for i in range(3):
        rows = slice((i + 1) * depth, (i + 2) * depth)
        moment = PARTICLE_MASS * vel[i]
        right[rows, 0:width] = (depth_w * moment + depth_s * entry(i, 2)).astype(BF16)
        right[rows, width : 2 * width] = (depth_w * entry(i, 0)).astype(BF16)
        right[rows, 2 * width : 3 * width] = (depth_w * entry(i, 1)).astype(BF16)
    total[0:edge] += lax.dot_general(tab[0:edge], right[...], NT, preferred_element_type=F32)


def gather_chunk(bases, offsets, vol, sizes, wide, tab, result, tables):
    size_x, size_y, depth = sizes
    width = bases.shape[1]
    weights, slopes = weights_of(offsets)
    build(bases, weights, slopes, size_x, size_y, tab, *tables)
    depth_w, depth_s = depth_tables(bases, weights, slopes, depth)
    result[...] = jnp.dot(wide[...], tab[...], preferred_element_type=F32)
    vel, aff = ([], [None] * 9)
    for i in range(3):
        rows = slice(i * depth, (i + 1) * depth)
        plain = result[rows, 0:width]
        vel.append(jnp.sum(plain * depth_w, 0, keepdims=True))
        aff[3 * i + 2] = 4.0 * jnp.sum(plain * depth_s, 0, keepdims=True)
        aff[3 * i] = 4.0 * jnp.sum(result[rows, width : 2 * width] * depth_w, 0, keepdims=True)
        aff[3 * i + 1] = 4.0 * jnp.sum(
            result[rows, 2 * width : 3 * width] * depth_w, 0, keepdims=True
        )
    vol = vol * (1.0 + TIME_STEP * (aff[0] + aff[4] + aff[8]))
    return (vel, aff, vol)


def take_rows(ref, lanes, count):
    return [ref[k : k + 1, lanes] for k in range(count)]


def first_kernel(sizes, counts, chunk, base, offset, vel, aff, vol, mask, place_in, take_out, wide, tab, right, total, xw, xs, yw, ys, *remote):
    greet(counts)
    total[...] = jnp.zeros_like(total)

    def body(step, carry):
        lanes = pl.ds(pl.multiple_of(step * chunk, chunk), chunk)
        scatter_chunk(
            base[:, 0, lanes], offset[:, 0, lanes], take_rows(vel, lanes, 3),
            take_rows(aff, lanes, 9), vol[:, lanes], sizes, tab.at[step], right.at[step],
            (xw, xs, yw, ys), total,
        )
        return carry

    lax.fori_loop(0, vel.shape[1] // chunk, body, 0)
    exchange(sizes, counts, mask, place_in, take_out, wide, tab, right, total, *remote)


def middle_kernel(sizes, counts, chunk, base, offset, vol, before, mask, place_in, take_out, wide, vol_out, seen, result, tab, right, total, xw, xs, yw, ys, *remote):
    greet(counts)
    total[...] = jnp.zeros_like(total)

    def body(step, carry):
        lanes = pl.ds(pl.multiple_of(step * chunk, chunk), chunk)
        vel, aff, ratio = gather_chunk(
            base[:, 0, lanes], offset[:, 0, lanes], vol[:, lanes], sizes, before, seen, result,
            (xw, xs, yw, ys),
        )
        vol_out[:, lanes] = ratio
        scatter_chunk(
            base[:, 1, lanes], offset[:, 1, lanes], vel, aff, ratio, sizes, tab.at[step],
            right.at[step], (xw, xs, yw, ys), total,
        )
        return carry

    lax.fori_loop(0, vol.shape[1] // chunk, body, 0)
    exchange(sizes, counts, mask, place_in, take_out, wide, tab, right, total, *remote)


def last_kernel(sizes, chunk, capacity, counts, base, offset, vol, wide, direction, out, tab, result, state, slots, xw, xs, yw, ys, buckets, got, sends, recvs):
    greet(counts)
    tables = (xw, xs, yw, ys)
    size_x, size_y, _ = sizes
    count_x, count_y = counts
    index_x = lax.axis_index("gx")
    index_y = lax.axis_index("gy")
    rows = vol.shape[1]

    def route(code):
        step_x = jnp.where(code < 3, -1, jnp.where(code > 5, 1, 0))
        step_y = code - 3 * step_x - 4
        to_x = step_x + index_x
        to_y = step_y + index_y
        inside = (to_x >= 0) & (to_x < count_x) & (to_y >= 0) & (to_y < count_y)
        return (
            jnp.where(inside, code, 4),
            jnp.where(inside, step_x, 0),
            jnp.where(inside, step_y, 0),
        )

    def body(step, carry):
        lanes = pl.ds(pl.multiple_of(step * chunk, chunk), chunk)
        bases = base[:, 1, lanes]
        offsets = offset[:, 1, lanes]
        vel, aff, ratio = gather_chunk(
            bases, offsets, vol[:, lanes], sizes, wide, tab, result, tables
        )
        moving, step_x, step_y = route(direction[:, lanes])
        shift = (step_x * size_x, step_y * size_y, None)
        for axis in range(3):
            spot = bases[axis : axis + 1].astype(F32) + offsets[axis : axis + 1]
            spot = spot + TIME_STEP * vel[axis]
            if shift[axis] is not None:
                spot = spot - shift[axis].astype(F32)
            state[axis : axis + 1, lanes] = spot
            state[3 + axis : 4 + axis, lanes] = vel[axis]
        for k in range(9):
            state[6 + k : 7 + k, lanes] = aff[k]
        state[15:16, lanes] = ratio
        out[:, lanes] = jnp.where(moving == 4, state[:, lanes], 0.0)
        return carry

    lax.fori_loop(0, rows // chunk, body, 0)

    parts = rows // LANES
    place = rows_iota(8)
    codes = jnp.where(place < 4, place, place + 1)
    hits = []
    for part in range(parts):
        moving, _, _ = route(direction[:, part * LANES : (part + 1) * LANES])
        hits.append(jnp.where(moving == codes, 1.0, 0.0))
    above = lax.broadcasted_iota(jnp.int32, (LANES, 2 * LANES), 0)
    along = lax.broadcasted_iota(jnp.int32, (LANES, 2 * LANES), 1)
    summer = jnp.where(above <= along, 1.0, 0.0).astype(BF16)
    sums = jnp.dot(jnp.concatenate(hits, 0).astype(BF16), summer, preferred_element_type=F32)
    before = (place * capacity).astype(F32)
    before = jnp.broadcast_to(before, (8, LANES))
    for part in range(parts):
        mine = slice(part * 8, (part + 1) * 8)
        slot = jnp.sum(hits[part] * (sums[mine, 0:LANES] + before), 0, keepdims=True) - 1.0
        slots[:, part * LANES : (part + 1) * LANES] = slot.astype(jnp.int32)
        before = before + sums[mine, LANES:]

    value = state[...]
    high = value.astype(BF16)
    rest = value - high.astype(F32)
    middle = rest.astype(BF16)
    low = (rest - middle.astype(F32)).astype(BF16)
    split = jnp.concatenate([high, middle, low], 0)
    for k in range(8):
        chosen = slots[...] - k * capacity == rows_iota(capacity)
        chosen = jnp.where(chosen, 1.0, 0.0).astype(BF16)
        packed = lax.dot_general(split, chosen, NT, preferred_element_type=F32)
        buckets[k] = packed[0:16] + packed[16:32] + packed[32:48]
    migrate(counts, buckets, out, got, sends, recvs)


def neighbour(counts, dx, dy):
    to_x = lax.axis_index("gx") + dx
    to_y = lax.axis_index("gy") + dy
    exists = (to_x >= 0) & (to_x < counts[0]) & (to_y >= 0) & (to_y < counts[1])
    return (exists, {"gx": to_x, "gy": to_y})


def greet(counts):
    barrier = pltpu.get_barrier_semaphore()
    for dx, dy in BLOCKS:
        exists, where = neighbour(counts, dx, dy)

        @pl.when(exists)
        def _():
            pl.semaphore_signal(
                barrier, inc=1, device_id=where, device_id_type=pl.DeviceIdType.MESH
            )


def await_peers(counts):
    barrier = pltpu.get_barrier_semaphore()
    peers = 0
    for dx, dy in BLOCKS:
        exists, _ = neighbour(counts, dx, dy)
        peers = peers + exists.astype(jnp.int32)
    pl.semaphore_wait(barrier, peers)


def transfers(counts, sign, source, target, send_sems, recv_sems):
    copies = []
    for k, (dx, dy) in enumerate(BLOCKS):
        exists, where = neighbour(counts, sign * dx, sign * dy)
        copy = pltpu.make_async_remote_copy(
            src_ref=source(k),
            dst_ref=target(k),
            send_sem=send_sems.at[k],
            recv_sem=recv_sems.at[k],
            device_id=where,
            device_id_type=pl.DeviceIdType.MESH,
        )
        comes, _ = neighbour(counts, -sign * dx, -sign * dy)
        copies.append((exists, comes, copy))
    return copies


def start_all(copies, target):
    for exists, _, copy in copies:
        pl.when(exists)(copy.start)
    for k, (_, comes, _) in enumerate(copies):

        @pl.when(jnp.logical_not(comes))
        def _():
            view = target(k)
            view[...] = jnp.zeros(view.shape, view.dtype)


def wait_all(copies):
    for _, comes, copy in copies:
        pl.when(comes)(copy.wait_recv)
    for exists, _, copy in copies:
        pl.when(exists)(copy.wait_send)


def pack_corners(value, channels, depth, spread):
    for k in range(4):
        for c in range(channels):
            spread[k * CORNER_ROWS + 4 * c : k * CORNER_ROWS + 4 * c + 4, :] = value(
                slice(k * CORNER_ROWS, k * CORNER_ROWS + 4), slice(c * depth, (c + 1) * depth)
            )


def unpack_corners(spread, channels, depth, square):
    square[...] = jnp.zeros_like(square)
    for k in range(4):
        for c in range(channels):
            square[
                k * CORNER_ROWS : k * CORNER_ROWS + 4, c * depth : (c + 1) * depth
            ] = spread[k * CORNER_ROWS + 4 * c : k * CORNER_ROWS + 4 * c + 4, :]


def exchange(sizes, counts, mask, place_in, take_out, wide, tab, right, total, margins, corners, got, got_corners, sent, sent_corners, halo, halo_corners, spread, square, speed, drawn, sends, recvs, sends_b, recvs_b):
    size_x, size_y, depth = sizes
    places, edge = block_rows(size_x, size_y)
    inner = places[4][0]

    def views(sides, tiles):
        def view(k):
            if k < 4:
                return sides.at[pl.ds(places[k][0], places[k][1])]
            return tiles.at[pl.ds((k - 4) * CORNER_ROWS, CORNER_ROWS)]

        return view

    margins[...] = total[0:inner].astype(BF16)

    def corner_of(rows, lanes):
        return total[inner + rows.start : inner + rows.stop, lanes]

    pack_corners(corner_of, 4, depth, spread)
    corners[...] = spread[...].astype(BF16)
    await_peers(counts)
    arriving = views(got, got_corners)
    copies = transfers(counts, 1, views(margins, corners), arriving, sends, recvs)
    start_all(copies, arriving)

    def body(step, carry):
        total[edge:] += lax.dot_general(
            tab[step, edge:], right[step], NT, preferred_element_type=F32
        )
        return carry

    lax.fori_loop(0, tab.shape[0], body, 0)
    wait_all(copies)
    spread[...] = got_corners[...].astype(F32)
    unpack_corners(spread, 4, depth, square)
    received = jnp.concatenate([got[...], square[...].astype(BF16)], 0)
    full = total[edge:] + jnp.dot(place_in[...], received, preferred_element_type=F32)
    mass = jnp.maximum(full[:, 0:depth], MASS_FLOOR)
    keep = (1 - mask[...]).astype(F32)
    for axis in range(3):
        value = full[:, (axis + 1) * depth : (axis + 2) * depth] / mass
        if axis == 2:
            value = value - TIME_STEP * GRAVITY
        speed[:, axis * depth : (axis + 1) * depth] = (value * keep).astype(BF16)
    drawn[...] = jnp.dot(take_out[...], speed[...], preferred_element_type=F32)
    sent[...] = drawn[0:inner].astype(BF16)

    def drawn_corner(rows, lanes):
        return drawn[inner + rows.start : inner + rows.stop, lanes]

    pack_corners(drawn_corner, 3, depth, spread)
    sent_corners[...] = spread[...].astype(BF16)
    arriving = views(halo, halo_corners)
    copies = transfers(counts, -1, views(sent, sent_corners), arriving, sends_b, recvs_b)
    start_all(copies, arriving)
    for axis in range(3):
        lanes = slice(axis * depth, (axis + 1) * depth)
        wide[lanes, edge:] = speed[:, lanes].astype(F32).T.astype(BF16)
    wait_all(copies)
    spread[...] = halo_corners[...].astype(F32)
    unpack_corners(spread, 3, depth, square)
    for axis in range(3):
        lanes = slice(axis * depth, (axis + 1) * depth)
        outer = jnp.concatenate([halo[:, lanes].astype(F32), square[:, lanes]], 0)
        wide[lanes, 0:edge] = outer.T.astype(BF16)


def migrate(counts, buckets, out, got, sends, recvs):
    capacity = buckets.shape[2]
    rows = out.shape[1] - 8 * capacity
    order = [0, 1, 2, 3, 5, 6, 7, 8]
    slot_of = [order.index(3 * (dx + 1) + dy + 1) for dx, dy in BLOCKS]

    def views(ref):
        return lambda k: ref.at[slot_of[k]]

    await_peers(counts)
    copies = transfers(counts, 1, views(buckets), views(got), sends, recvs)
    start_all(copies, views(got))
    wait_all(copies)
    for k in range(8):
        out[:, rows + k * capacity : rows + (k + 1) * capacity] = got[k]


def vmem(count):
    return [pl.BlockSpec(memory_space=pltpu.VMEM)] * count


def per_device(counts, base, offset, velocity, affine, volume, node_mask, direction):
    sizes = node_mask.shape
    size_x, size_y, depth = sizes
    rows = velocity.shape[1]
    capacity = rows // 16
    chunk = min(rows, 512)
    _, edge = block_rows(size_x, size_y)
    cells = size_x * size_y
    all_rows = edge + cells
    base = jnp.swapaxes(base, 0, 1)
    offset = jnp.swapaxes(offset, 0, 1)
    volume = volume.reshape(1, rows)
    direction = direction.reshape(1, rows)
    mask = node_mask.reshape(cells, depth)
    owners = owner_rows(size_x, size_y)
    choose = (owners[:, None] == np.arange(cells)[None]).astype(np.float32)
    take_out = jnp.asarray(choose, BF16)
    place_in = jnp.asarray(choose.T, BF16)

    inner = edge - 4 * CORNER_ROWS
    steps = rows // chunk
    seen = pltpu.VMEM((all_rows, 3 * chunk), BF16)
    result = pltpu.VMEM((3 * depth, 3 * chunk), F32)
    tables = [pltpu.VMEM((size_x + 8, chunk), F32)] * 2 + [pltpu.VMEM((size_y + 8, chunk), F32)] * 2
    spread = [
        pltpu.VMEM((steps, all_rows, 3 * chunk), BF16),
        pltpu.VMEM((steps, 4 * depth, 3 * chunk), BF16),
        pltpu.VMEM((all_rows, 4 * depth), F32),
    ] + tables
    remote = [
        pltpu.VMEM((inner, 4 * depth), BF16),
        pltpu.VMEM((4 * CORNER_ROWS, depth), BF16),
        pltpu.VMEM((inner, 4 * depth), BF16),
        pltpu.VMEM((4 * CORNER_ROWS, depth), BF16),
        pltpu.VMEM((inner, 3 * depth), BF16),
        pltpu.VMEM((4 * CORNER_ROWS, depth), BF16),
        pltpu.VMEM((inner, 3 * depth), BF16),
        pltpu.VMEM((4 * CORNER_ROWS, depth), BF16),
        pltpu.VMEM((4 * CORNER_ROWS, depth), F32),
        pltpu.VMEM((4 * CORNER_ROWS, 4 * depth), F32),
        pltpu.VMEM((cells, 3 * depth), BF16),
        pltpu.VMEM((edge, 3 * depth), F32),
    ] + [pltpu.SemaphoreType.DMA((8,))] * 4
    wide_out = jax.ShapeDtypeStruct((3 * depth, all_rows), BF16)

    def params(number):
        return pltpu.CompilerParams(
            collective_id=number, has_side_effects=True, vmem_limit_bytes=56 * 1024 * 1024
        )

    wide = pl.pallas_call(
        functools.partial(first_kernel, sizes, counts, chunk),
        out_shape=wide_out,
        in_specs=vmem(8),
        out_specs=vmem(1)[0],
        scratch_shapes=spread + remote,
        compiler_params=params(0),
        name="scatter",
    )(base, offset, velocity, affine, volume, mask, place_in, take_out)
    wide, volume = pl.pallas_call(
        functools.partial(middle_kernel, sizes, counts, chunk),
        out_shape=[wide_out, jax.ShapeDtypeStruct((1, rows), F32)],
        in_specs=vmem(7),
        out_specs=vmem(2),
        scratch_shapes=[seen, result] + spread + remote,
        compiler_params=params(1),
        name="gather_scatter",
    )(base, offset, volume, wide, mask, place_in, take_out)
    return pl.pallas_call(
        functools.partial(last_kernel, sizes, chunk, capacity, counts),
        out_shape=jax.ShapeDtypeStruct((16, rows + 8 * capacity), F32),
        in_specs=vmem(5),
        out_specs=vmem(1)[0],
        scratch_shapes=[seen, result, pltpu.VMEM((16, rows), F32), pltpu.VMEM((1, rows), jnp.int32)]
        + tables
        + [pltpu.VMEM((8, 16, capacity), F32)] * 2
        + [pltpu.SemaphoreType.DMA((8,))] * 2,
        compiler_params=params(2),
        name="gather_pack",
    )(base, offset, volume, wide, direction)


def solution(mesh):
    counts = (mesh.shape["gx"], mesh.shape["gy"])
    placed = (
        P(None, None, ("gx", "gy")),
        P(None, None, ("gx", "gy")),
        P(None, ("gx", "gy")),
        P(None, ("gx", "gy")),
        P(("gx", "gy")),
        P("gx", "gy", None),
        P(("gx", "gy")),
    )
    return jax.shard_map(
        functools.partial(per_device, counts),
        mesh=mesh,
        in_specs=placed,
        out_specs=P(None, ("gx", "gy")),
        check_vma=False,
    )
```
